16 devices in a mesh: dp: 2 (over y, z), ep: 8 (over x, core).
Axes of the slice: x: 4, y: 2, z: 1, core: 2. Of those that a mesh axis runs over, the one named last changes fastest.
The devices are a block of a 4x4x8 slice.
Arguments:
- dispatched: bfloat16 [16, 64, 96, 2048], P('dp', 'ep'), parts along dimension 0
- w_gate: bfloat16 [64, 2048, 1408], P('ep')
- w_up: bfloat16 [64, 2048, 1408], P('ep')
- w_down: bfloat16 [64, 1408, 2048], P('ep')
- fill_count: int32 [16, 64], P('dp', 'ep'), parts along dimension 0
- slot_index: int32 [8192, 6], P(('dp', 'ep')), parts along dimension 0
- expert_id: int32 [8192, 6], P(('dp', 'ep')), parts along dimension 0
- gate_weight: float32 [8192, 6], P(('dp', 'ep')), parts along dimension 0
Outputs:
- output: bfloat16 [8192, 2048], P(('dp', 'ep')), parts along dimension 0
There are 2 independent parts. The reference program is written for one: setup_inputs(seed, part) draws one part's arguments, and reference() takes and returns one part's arrays. A program takes and returns all parts, laid end to end along the dimension named above; an argument that names none is the same for every part.
All inputs are finite; a program needn't handle non-finite values.
Results may differ from the reference program's by a relative error of at most 0.00126.
Values are sent between devices in bfloat16 or wider.
A program may use at most 768 MiB of HBM per device.

```python
import jax
import jax.numpy as jnp
from jax import lax

HIDDEN = 2048
FFN_DIM = 1408
EXPERTS = 64
TOP_K = 6
TOKENS_DEV = 512
GROUP_SIZE = 8
CAPACITY = (2 * TOKENS_DEV * TOP_K) // EXPERTS


def draw_routing(route_key):
    key_perm, key_noise, key_shift = jax.random.split(route_key, 3)
    popularity = jax.random.permutation(key_perm, EXPERTS)
    base_score = 4000 // (popularity + 1)
    noise_term = jax.random.randint(key_noise, (GROUP_SIZE, TOKENS_DEV, EXPERTS), 0, 1000)
    cover_shift = jax.random.randint(key_shift, (GROUP_SIZE, 1), 0, EXPERTS)
    expert_ids = jnp.arange(EXPERTS, dtype=jnp.int32)
    cover_id = (jnp.arange(TOKENS_DEV, dtype=jnp.int32)[None, :] + cover_shift) % EXPERTS
    cover_bonus = jnp.where(expert_ids[None, None, :] == cover_id[:, :, None], 100000, 0)
    route_score = (base_score[None, None, :] + noise_term + cover_bonus) * EXPERTS + expert_ids
    chosen = lax.top_k(route_score, TOP_K)[1]
    onehot = (chosen.reshape(GROUP_SIZE, TOKENS_DEV * TOP_K, 1) == expert_ids).astype(jnp.int32)
    earlier = jnp.cumsum(onehot, axis=1) - onehot
    arrival = jnp.sum(earlier * onehot, axis=2)
    slot_index = jnp.where(arrival < CAPACITY, arrival, -1)
    filled_count = jnp.minimum(jnp.sum(onehot, axis=1), CAPACITY)
    expert_id = chosen.reshape(GROUP_SIZE * TOKENS_DEV, TOP_K).astype(jnp.int32)
    slot_index = slot_index.reshape(GROUP_SIZE * TOKENS_DEV, TOP_K).astype(jnp.int32)
    return expert_id, slot_index, filled_count.astype(jnp.int32)


def setup_inputs(seed: int = 0, part: int = 0) -> dict:
    shared_key, part_root = jax.random.split(jax.random.key(seed))
    key_gate_w, key_up_w, key_down_w = jax.random.split(shared_key, 3)
    part_key = jax.random.fold_in(part_root, part)
    key_route, key_rows, key_mix = jax.random.split(part_key, 3)
    expert_id, slot_index, filled_count = draw_routing(key_route)
    dispatched = jax.random.normal(key_rows, (GROUP_SIZE, EXPERTS, CAPACITY, HIDDEN), jnp.float32)
    w_gate = jax.random.normal(key_gate_w, (EXPERTS, HIDDEN, FFN_DIM), jnp.float32) * HIDDEN ** -0.5
    w_up = jax.random.normal(key_up_w, (EXPERTS, HIDDEN, FFN_DIM), jnp.float32) * HIDDEN ** -0.5
    w_down = jax.random.normal(key_down_w, (EXPERTS, FFN_DIM, HIDDEN), jnp.float32) * FFN_DIM ** -0.5
    logits = jax.random.normal(key_mix, (GROUP_SIZE * TOKENS_DEV, TOP_K), jnp.float32) * 1.5
    return {
        "dispatched": dispatched.astype(jnp.bfloat16),
        "w_gate": w_gate.astype(jnp.bfloat16),
        "w_up": w_up.astype(jnp.bfloat16),
        "w_down": w_down.astype(jnp.bfloat16),
        "fill_count": filled_count,
        "slot_index": slot_index,
        "expert_id": expert_id,
        "gate_weight": jax.nn.softmax(logits, axis=-1),
    }


def reference(dispatched, w_gate, w_up, w_down, fill_count, slot_index, expert_id, gate_weight):
    group_size = dispatched.shape[0]
    capacity = dispatched.shape[2]
    tokens_dev = slot_index.shape[0] // group_size

    def expert_ffn(operands):
        row_block, gate_w, up_w, down_w, filled = operands
        rows_f32 = row_block.astype(jnp.float32)
        pre_gate = jnp.einsum("scd,df->scf", rows_f32, gate_w.astype(jnp.float32))
        pre_up = jnp.einsum("scd,df->scf", rows_f32, up_w.astype(jnp.float32))
        hidden = (jax.nn.silu(pre_gate) * pre_up).astype(jnp.bfloat16)
        result = jnp.einsum("scf,fd->scd", hidden.astype(jnp.float32), down_w.astype(jnp.float32)).astype(jnp.bfloat16)
        live_mask = jnp.arange(capacity)[None, :] < filled[:, None]
        return jnp.where(live_mask[:, :, None], result, jnp.zeros_like(result))

    expert_out = lax.map(expert_ffn, (jnp.swapaxes(dispatched, 0, 1), w_gate, w_up, w_down, jnp.swapaxes(fill_count, 0, 1)))
    flat_rows = expert_out.reshape(-1, expert_out.shape[-1])
    source = (jnp.arange(slot_index.shape[0]) // tokens_dev)[:, None]
    row_index = (expert_id * group_size + source) * capacity + jnp.maximum(slot_index, 0)
    weight = jnp.where(slot_index >= 0, gate_weight, 0.0)
    combined = jnp.zeros((slot_index.shape[0], flat_rows.shape[1]), jnp.float32)
    for choice in range(slot_index.shape[1]):
        picked = jnp.take(flat_rows, row_index[:, choice], axis=0).astype(jnp.float32)
        combined = combined + weight[:, choice, None] * picked
    return combined.astype(jnp.bfloat16)
```

```python
import functools

import jax
import jax.numpy as jnp
from jax import lax
from jax.experimental import pallas as pl
from jax.experimental.pallas import tpu as pltpu
from jax.sharding import PartitionSpec as P

MESH = pl.DeviceIdType.MESH
SUB = 8
TILE = 256
KB = 128
STRIDE = 1024
VMEM_LIMIT = 66 * 1000 * 1000


def barrier(group):
    me = lax.axis_index("ep")
    sem = pltpu.get_barrier_semaphore()
    for o in range(1, group):
        pl.semaphore_signal(sem, inc=1, device_id={"ep": lax.rem(me + o, group)}, device_id_type=MESH)
    pl.semaphore_wait(sem, group - 1)


def counts_kernel(group, fill_ref, all_ref, send_sem, recv_sem, own_sem):
    me = lax.axis_index("ep")
    barrier(group)
    own = pltpu.make_async_copy(fill_ref, all_ref.at[me], own_sem)
    own.start()
    copies = []
    for o in range(1, group):
        to = lax.rem(me + o, group)
        copy = pltpu.make_async_remote_copy(
            fill_ref, all_ref.at[me], send_sem.at[o], recv_sem.at[o], device_id={"ep": to}, device_id_type=MESH)
        copy.start()
        copies.append(copy)
    own.wait()
    for copy in copies:
        copy.wait()


def exchange_counts(fill_count, group):
    block = jnp.pad(fill_count, ((0, 0), (0, 128 - fill_count.shape[1])))
    return pl.pallas_call(
        functools.partial(counts_kernel, group),
        out_shape=jax.ShapeDtypeStruct((group,) + block.shape, jnp.int32),
        in_specs=[pl.BlockSpec(memory_space=pltpu.VMEM)],
        out_specs=pl.BlockSpec(memory_space=pltpu.HBM),
        scratch_shapes=[pltpu.SemaphoreType.DMA((group,)), pltpu.SemaphoreType.DMA((group,)), pltpu.SemaphoreType.DMA],
        compiler_params=pltpu.CompilerParams(collective_id=0, has_side_effects=True),
        name="counts",
    )(block)


def ffn_kernel(S, E, fill_ref, x_hbm, wg_hbm, wu_hbm, wd_hbm, y_hbm,
               xb, wg, wu, wd, hb, yb, live, pos, x_sem, w_sem, y_sem):
    F = wg.shape[2]
    D = wg.shape[1]
    half = (F // 128 // 2) * 128
    parts = ((0, half), (half, F - half))

    def blocks(s, e):
        return (fill_ref[s, e] + SUB - 1) // SUB

    def weight_copies(e, slot):
        out = []
        for p, (a, n) in enumerate(parts):
            cols = pl.ds(a, n)
            out.append(pltpu.make_async_copy(wg_hbm.at[e, :, cols], wg.at[slot, :, cols], w_sem.at[slot, 2 * p]))
            out.append(pltpu.make_async_copy(wu_hbm.at[e, :, cols], wu.at[slot, :, cols], w_sem.at[slot, 2 * p + 1]))
        out.append(pltpu.make_async_copy(wd_hbm.at[e], wd.at[slot], w_sem.at[slot, 4]))
        return out

    def row_copies(e, slot):
        out, at = [], 0
        for s in range(S):
            n = blocks(s, e)
            out.append(pltpu.make_async_copy(
                x_hbm.at[s, e, pl.ds(0, n)], xb.at[slot, pl.ds(at, n)], x_sem.at[slot, s]))
            at = at + n
        return out, at

    def result_copies(e, slot, read_pos):
        out, at = [], 0
        for s in range(S):
            n = blocks(s, e)
            out.append(pltpu.make_async_copy(
                yb.at[slot, pl.ds(at, n)], y_hbm.at[s, pl.ds(read_pos(s), n)], y_sem.at[slot, s]))
            at = at + n
        return out

    def fetch(e, slot):
        copies, _ = row_copies(e, slot)
        for c in copies:
            c.start()
        for c in weight_copies(e, slot):
            c.start()

    fetch(0, 0)
    for s in range(S):
        pos[0, s] = 0

    def expert(e, carry):
        slot = lax.rem(e, 2)

        @pl.when(e + 1 < E)
        def _():
            fetch(e + 1, 1 - slot)

        copies, total = row_copies(e, slot)
        for c in copies:
            c.wait()
        weights = weight_copies(e, slot)

        @pl.when(e >= 2)
        def _():
            for c in result_copies(e - 2, slot, lambda s: pos[1 + slot, s]):
                c.wait()

        rows = total * SUB

        def up_part(b0, tile, p):
            a0, n = parts[p]
            nb = tile // SUB
            for c in range(a0 // 128, (a0 + n) // 128):
                cols = pl.ds(c * 128, 128)
                x = xb[slot, pl.ds(b0, nb)].reshape(tile, D)
                w = jnp.concatenate([wg[slot, :, cols], wu[slot, :, cols]], axis=1)
                ab = jnp.dot(x, w, preferred_element_type=jnp.float32)
                a, b = ab[:, :128], ab[:, 128:]
                h = jnp.where(live[pl.ds(0, tile), :] > 0, a * jax.nn.sigmoid(a) * b, 0.0)
                hb[pl.ds(0, tile), cols] = h.astype(jnp.bfloat16)

        def down(b0, tile):
            nb = tile // SUB
            for c in range(D // 256):
                cols = pl.ds(c * 256, 256)
                y = jnp.dot(hb[pl.ds(0, tile), :], wd[slot, :, cols], preferred_element_type=jnp.float32)
                yb[slot, pl.ds(b0, nb), :, cols] = y.astype(jnp.bfloat16).reshape(nb, SUB, 256)

        def mask(b0, tile):
            row = lax.broadcasted_iota(jnp.int32, (tile, 128), 0) + b0 * SUB
            ok = jnp.zeros((tile, 128), jnp.int32)
            at = 0
            for s in range(S):
                ok = jnp.where((row >= at * SUB) & (row < at * SUB + fill_ref[s, e]), 1, ok)
                at = at + blocks(s, e)
            live[pl.ds(0, tile), :] = ok

        def run(b0, tile, first):
            mask(b0, tile)
            for p in range(2):
                @pl.when(first)
                def _():
                    weights[2 * p].wait()
                    weights[2 * p + 1].wait()
                up_part(b0, tile, p)

            @pl.when(first)
            def _():
                weights[4].wait()
            down(b0, tile)

        big = (rows + TILE - 1 - TILE // 2) // TILE

        def body(i, c):
            run(i * (TILE // SUB), TILE, i == 0)
            return c

        lax.fori_loop(0, big, body, 0)

        @pl.when(big * TILE < rows)
        def _():
            run(big * (TILE // SUB), TILE // 2, big == 0)

        for s in range(S):
            pos[1 + slot, s] = pos[0, s]
        for c in result_copies(e, slot, lambda s: pos[1 + slot, s]):
            c.start()
        for s in range(S):
            pos[0, s] = pos[0, s] + blocks(s, e)
        return carry

    lax.fori_loop(0, E, expert, 0)
    for e in (E - 2, E - 1):
        for c in result_copies(e, e % 2, lambda s: pos[1 + e % 2, s]):
            c.wait()


def ffn(dispatched, w_gate, w_up, w_down, fill_count):
    S, E, C, D = dispatched.shape
    F = w_gate.shape[2]
    nb = S * C // SUB + TILE // SUB
    anyspec = pl.BlockSpec(memory_space=pltpu.HBM)
    return pl.pallas_call(
        functools.partial(ffn_kernel, S, E),
        out_shape=jax.ShapeDtypeStruct((S, E * C // SUB, SUB, D), jnp.bfloat16),
        in_specs=[pl.BlockSpec(memory_space=pltpu.SMEM)] + [anyspec] * 4,
        out_specs=anyspec,
        scratch_shapes=[
            pltpu.VMEM((2, nb, SUB, D), jnp.bfloat16),
            pltpu.VMEM((2, D, F), jnp.bfloat16),
            pltpu.VMEM((2, D, F), jnp.bfloat16),
            pltpu.VMEM((2, F, D), jnp.bfloat16),
            pltpu.VMEM((TILE, F), jnp.bfloat16),
            pltpu.VMEM((2, nb, SUB, D), jnp.bfloat16),
            pltpu.VMEM((TILE, 128), jnp.int32),
            pltpu.SMEM((3, S), jnp.int32),
            pltpu.SemaphoreType.DMA((2, S)),
            pltpu.SemaphoreType.DMA((2, 5)),
            pltpu.SemaphoreType.DMA((2, S)),
        ],
        compiler_params=pltpu.CompilerParams(vmem_limit_bytes=VMEM_LIMIT),
        cost_estimate=pl.CostEstimate(flops=6 * S * C * E * D * F // 4, bytes_accessed=6 * E * D * F, transcendentals=0),
        name="ffn",
    )(fill_count, dispatched.reshape(S, E, C // SUB, SUB, D), w_gate, w_up, w_down)


def return_kernel(M, group, E, counts, expert_ref, slot_ref, weight_ref, y_hbm, out_ref,
                  rb, acc, idx, send_sem, recv_sem, own_sem):
    me = lax.axis_index("ep")
    barrier(group)
    own = pltpu.make_async_copy(y_hbm.at[me, pl.ds(0, M // SUB)], rb.at[0], own_sem)
    own.start()
    copies = []
    for o in range(1, group):
        to = lax.rem(me + o, group)
        copies.append(pltpu.make_async_remote_copy(
            y_hbm.at[to, pl.ds(0, M // SUB)], rb.at[o], send_sem.at[o], recv_sem.at[o],
            device_id={"ep": to}, device_id_type=MESH))
    for copy in copies:
        copy.start()

    ids, place = expert_ref[...], slot_ref[...]
    number = jnp.full(ids.shape, -STRIDE * group * 2, jnp.int32)
    for d in range(group):
        at = d * STRIDE
        for e in range(E):
            number = jnp.where(ids == d * E + e, at, number)
            at = at + (counts[d, me, e] + SUB - 1) // SUB * SUB
    idx[...] = jnp.where(place >= 0, number + place, -1)
    acc[...] = jnp.zeros_like(acc)
    T, D = acc.shape
    J = ids.shape[0]

    def combine(o):
        d = lax.rem(me - o + group, group)
        total = 0
        for e in range(E):
            total = total + (counts[d, me, e] + SUB - 1) // SUB * SUB

        def block(i, c):
            r0 = jnp.minimum(i * KB, M - KB)
            row = lax.broadcasted_iota(jnp.int32, (KB, T), 0) + r0
            row = jnp.where(row >= i * KB, row + d * STRIDE, -2)
            w = jnp.zeros((KB, T), jnp.float32)
            for j in range(J):
                w = jnp.where(row == idx[j:j + 1, :], weight_ref[j:j + 1, :], w)
            hi = w.astype(jnp.bfloat16)
            rest = w - hi.astype(jnp.float32)
            mid = rest.astype(jnp.bfloat16)
            lo = (rest - mid.astype(jnp.float32)).astype(jnp.bfloat16)
            p3 = jnp.concatenate([hi, mid, lo], axis=0)
            alive = lax.broadcasted_iota(jnp.int32, (KB, 256), 0) + r0 < total
            for n in range(D // 256):
                cols = pl.ds(n * 256, 256)
                y = rb[o, pl.ds(r0 // SUB, KB // SUB), :, cols].reshape(KB, 256)
                y = jnp.where(alive, y.astype(jnp.float32), 0.0).astype(jnp.bfloat16)
                y3 = jnp.concatenate([y, y, y], axis=0)
                acc[:, cols] += lax.dot_general(p3, y3, (((0,), (0,)), ((), ())), preferred_element_type=jnp.float32)
            return c
        lax.fori_loop(0, -(-M // KB), block, 0)

    own.wait()
    combine(0)

    def step(o, c):
        copy = pltpu.make_async_remote_copy(
            y_hbm.at[0, pl.ds(0, M // SUB)], rb.at[o], send_sem.at[o], recv_sem.at[o],
            device_id={"ep": lax.rem(me + o, group)}, device_id_type=MESH)
        copy.wait()
        combine(o)
        return c

    lax.fori_loop(1, group, step, 0)
    out_ref[...] = acc[...].astype(out_ref.dtype)


def return_rows(M, cid, counts, y, expert_id, slot_index, gate_weight):
    group, _, E = counts.shape
    J, T = expert_id.shape
    D = y.shape[-1]
    vmem = pl.BlockSpec(memory_space=pltpu.VMEM)
    return pl.pallas_call(
        functools.partial(return_kernel, M, group, E),
        out_shape=jax.ShapeDtypeStruct((T, D), jnp.bfloat16),
        in_specs=[pl.BlockSpec(memory_space=pltpu.SMEM), vmem, vmem, vmem, pl.BlockSpec(memory_space=pltpu.HBM)],
        out_specs=vmem,
        scratch_shapes=[
            pltpu.VMEM((group, M // SUB, SUB, D), jnp.bfloat16),
            pltpu.VMEM((T, D), jnp.float32),
            pltpu.VMEM((J, T), jnp.int32),
            pltpu.SemaphoreType.DMA((group,)),
            pltpu.SemaphoreType.DMA((group,)),
            pltpu.SemaphoreType.DMA,
        ],
        compiler_params=pltpu.CompilerParams(collective_id=cid, has_side_effects=True, vmem_limit_bytes=VMEM_LIMIT),
        name="return_%d" % M,
    )(counts, expert_id, slot_index, gate_weight, y)


BOUNDS = (192, 240, 256, 272, 288, 304, 320, 336, 352, 376, 416, 512, 768)


def solution(mesh):
    group = mesh.shape["ep"]

    def local_step(dispatched, w_gate, w_up, w_down, fill_count, slot_index, expert_id, gate_weight):
        E, C = dispatched.shape[1:3]
        counts = exchange_counts(fill_count, group)[:, :, :E]
        y = ffn(dispatched, w_gate, w_up, w_down, fill_count)
        most = jnp.max(jnp.sum((counts + SUB - 1) // SUB * SUB, axis=2))
        bounds = tuple(b for b in BOUNDS if b < E * C) + (E * C,)
        which = jnp.sum((most > jnp.array(bounds[:-1], jnp.int32)).astype(jnp.int32))
        branches = [functools.partial(return_rows, b, 1 + i) for i, b in enumerate(bounds)]
        return lax.switch(which, branches, counts, y, expert_id.T, slot_index.T, gate_weight.T)

    token_spec = P(("dp", "ep"))
    in_specs = (P("dp", "ep"), P("ep"), P("ep"), P("ep"), P("dp", "ep"), token_spec, token_spec, token_spec)
    return jax.shard_map(local_step, mesh=mesh, in_specs=in_specs, out_specs=token_spec, check_vma=False)
```

```python
import functools

import jax
import jax.numpy as jnp
from jax import lax
from jax.experimental import pallas as pl
from jax.experimental.pallas import tpu as pltpu
from jax.sharding import PartitionSpec as P

MESH = pl.DeviceIdType.MESH
SUB = 8
TILES = (384, 256, 128)
TILE = TILES[0]
CUTS = (0, 256, 768, 1 << 30)
KB = 128
STRIDE = 1024
VMEM_LIMIT = 66 * 1000 * 1000


def barrier(group):
    me = lax.axis_index("ep")
    sem = pltpu.get_barrier_semaphore()
    for o in range(1, group):
        pl.semaphore_signal(sem, inc=1, device_id={"ep": lax.rem(me + o, group)}, device_id_type=MESH)
    pl.semaphore_wait(sem, group - 1)


def counts_kernel(group, fill_ref, all_ref, send_sem, recv_sem, own_sem):
    me = lax.axis_index("ep")
    barrier(group)
    own = pltpu.make_async_copy(fill_ref, all_ref.at[me], own_sem)
    own.start()
    copies = []
    for o in range(1, group):
        to = lax.rem(me + o, group)
        copy = pltpu.make_async_remote_copy(
            fill_ref, all_ref.at[me], send_sem.at[o], recv_sem.at[o], device_id={"ep": to}, device_id_type=MESH)
        copy.start()
        copies.append(copy)
    own.wait()
    for copy in copies:
        copy.wait()


def exchange_counts(fill_count, group):
    block = jnp.pad(fill_count, ((0, 0), (0, 128 - fill_count.shape[1])))
    return pl.pallas_call(
        functools.partial(counts_kernel, group),
        out_shape=jax.ShapeDtypeStruct((group,) + block.shape, jnp.int32),
        in_specs=[pl.BlockSpec(memory_space=pltpu.VMEM)],
        out_specs=pl.BlockSpec(memory_space=pltpu.HBM),
        scratch_shapes=[pltpu.SemaphoreType.DMA((group,)), pltpu.SemaphoreType.DMA((group,)), pltpu.SemaphoreType.DMA],
        compiler_params=pltpu.CompilerParams(collective_id=0, has_side_effects=True),
        name="counts",
    )(block)


def ffn_kernel(S, E, i0, i1, fill_ref, x_hbm, wg_hbm, wu_hbm, wd_hbm, y_hbm,
               xb, wg, wu, wd, hb, yb, live, pos, order, x_sem, w_sem, y_sem):
    F = wg.shape[2]
    D = wg.shape[1]
    parts = tuple((p, min(F, q) - p) for p, q in zip(CUTS, CUTS[1:]) if p < F)

    def blocks(s, e):
        return (fill_ref[s, e] + SUB - 1) // SUB

    held = [functools.reduce(lambda u, v: u + v, [blocks(s, e) for s in range(S)]) for e in range(E)]
    for e in range(E):
        rank = 0
        for k in range(E):
            if k != e:
                ahead = held[k] >= held[e] if k < e else held[k] > held[e]
                rank = rank + ahead.astype(jnp.int32)
        order[rank] = e

    def weight_copies(e, slot):
        out = []
        for p, (a, n) in enumerate(parts):
            cols = pl.ds(a, n)
            out.append(pltpu.make_async_copy(wg_hbm.at[e, :, cols], wg.at[slot, :, cols], w_sem.at[slot, 2 * p]))
            out.append(pltpu.make_async_copy(wu_hbm.at[e, :, cols], wu.at[slot, :, cols], w_sem.at[slot, 2 * p + 1]))
        out.append(pltpu.make_async_copy(wd_hbm.at[e], wd.at[slot], w_sem.at[slot, 2 * len(parts)]))
        return out

    def row_copies(e, slot):
        out, at = [], 0
        for s in range(S):
            n = blocks(s, e)
            out.append(pltpu.make_async_copy(
                x_hbm.at[s, e, pl.ds(0, n)], xb.at[slot, pl.ds(at, n)], x_sem.at[slot, s]))
            at = at + n
        return out, at

    def result_copies(e, slot, read_pos):
        out, at = [], 0
        for s in range(S):
            n = blocks(s, e)
            out.append(pltpu.make_async_copy(
                yb.at[slot, pl.ds(at, n)], y_hbm.at[s, pl.ds(read_pos(s), n)], y_sem.at[slot, s]))
            at = at + n
        return out

    def fetch(e, slot):
        copies, _ = row_copies(e, slot)
        for c in copies:
            c.start()
        for c in weight_copies(e, slot):
            c.start()

    fetch(order[i0], 0)
    for s in range(S):
        pos[0, s] = 0

    def expert(i, carry):
        e = order[i]
        slot = lax.rem(i - i0, 2)

        @pl.when(i + 1 < i1)
        def _():
            fetch(order[i + 1], 1 - slot)

        copies, total = row_copies(e, slot)
        for c in copies:
            c.wait()
        weights = weight_copies(e, slot)

        @pl.when(i >= i0 + 2)
        def _():
            for c in result_copies(order[i - 2], slot, lambda s: pos[1 + slot, s]):
                c.wait()

        rows = total * SUB

        def up_part(b0, tile, p):
            a0, n = parts[p]
            nb = tile // SUB
            c = a0
            while c < a0 + n:
                k = min(256, a0 + n - c)
                cols = pl.ds(c, k)
                x = xb[slot, pl.ds(b0, nb)].reshape(tile, D)
                w = jnp.concatenate([wg[slot, :, cols], wu[slot, :, cols]], axis=1)
                ab = jnp.dot(x, w, preferred_element_type=jnp.float32)
                on = live[pl.ds(0, tile), :] > 0
                for q in range(0, k, 128):
                    a, b = ab[:, q:q + 128], ab[:, k + q:k + q + 128]
                    h = jnp.where(on, a * jax.nn.sigmoid(a) * b, 0.0)
                    hb[pl.ds(0, tile), pl.ds(c + q, 128)] = h.astype(jnp.bfloat16)
                c += k

        def down(b0, tile):
            nb = tile // SUB
            for c in range(D // 256):
                cols = pl.ds(c * 256, 256)
                y = jnp.dot(hb[pl.ds(0, tile), :], wd[slot, :, cols], preferred_element_type=jnp.float32)
                yb[slot, pl.ds(b0, nb), :, cols] = y.astype(jnp.bfloat16).reshape(nb, SUB, 256)

        def mask(b0, tile):
            row = lax.broadcasted_iota(jnp.int32, (tile, 128), 0) + b0 * SUB
            ok = jnp.zeros((tile, 128), jnp.int32)
            at = 0
            for s in range(S):
                ok = jnp.where((row >= at * SUB) & (row < at * SUB + fill_ref[s, e]), 1, ok)
                at = at + blocks(s, e)
            live[pl.ds(0, tile), :] = ok

        def run(b0, tile, first):
            mask(b0, tile)
            for p in range(len(parts)):
                @pl.when(first)
                def _():
                    weights[2 * p].wait()
                    weights[2 * p + 1].wait()

                up_part(b0, tile, p)

            @pl.when(first)
            def _():
                weights[2 * len(parts)].wait()

            down(b0, tile)

        big = (rows + TILE - 1 - TILES[1]) // TILE
        rest = rows - big * TILE

        def body(i, c):
            run(i * (TILE // SUB), TILE, i == 0)
            return c

        lax.fori_loop(0, big, body, 0)
        for tile, under in zip(TILES[1:], TILES[2:] + (0,)):
            @pl.when((rest > under) & (rest <= tile))
            def _():
                run(big * (TILE // SUB), tile, big == 0)

        for s in range(S):
            pos[1 + slot, s] = pos[0, s]
        for c in result_copies(e, slot, lambda s: pos[1 + slot, s]):
            c.start()
        for s in range(S):
            pos[0, s] = pos[0, s] + blocks(s, e)
        return carry

    lax.fori_loop(i0, i1, expert, 0)
    for i in range(max(i0, i1 - 2), i1):
        for c in result_copies(order[i], (i - i0) % 2, lambda s: pos[1 + (i - i0) % 2, s]):
            c.wait()


def ffn(i0, i1, dispatched, w_gate, w_up, w_down, fill_count):
    S, E, C, D = dispatched.shape
    F = w_gate.shape[2]
    nb = S * C // SUB + TILE // SUB
    parts = sum(1 for c in CUTS[:-1] if c < F)
    slots = min(2, i1 - i0)
    anyspec = pl.BlockSpec(memory_space=pltpu.HBM)
    return pl.pallas_call(
        functools.partial(ffn_kernel, S, E, i0, i1),
        out_shape=jax.ShapeDtypeStruct((S, (i1 - i0) * C // SUB, SUB, D), jnp.bfloat16),
        in_specs=[pl.BlockSpec(memory_space=pltpu.SMEM)] + [anyspec] * 4,
        out_specs=anyspec,
        scratch_shapes=[
            pltpu.VMEM((slots, nb, SUB, D), jnp.bfloat16),
            pltpu.VMEM((slots, D, F), jnp.bfloat16),
            pltpu.VMEM((slots, D, F), jnp.bfloat16),
            pltpu.VMEM((slots, F, D), jnp.bfloat16),
            pltpu.VMEM((TILE, F), jnp.bfloat16),
            pltpu.VMEM((slots, nb, SUB, D), jnp.bfloat16),
            pltpu.VMEM((TILE, 128), jnp.int32),
            pltpu.SMEM((3, S), jnp.int32),
            pltpu.SMEM((E,), jnp.int32),
            pltpu.SemaphoreType.DMA((2, S)),
            pltpu.SemaphoreType.DMA((2, 2 * parts + 1)),
            pltpu.SemaphoreType.DMA((2, S)),
        ],
        compiler_params=pltpu.CompilerParams(vmem_limit_bytes=VMEM_LIMIT),
        cost_estimate=pl.CostEstimate(
            flops=6 * S * C * (i1 - i0) * D * F // 2, bytes_accessed=6 * (i1 - i0) * D * F, transcendentals=0),
    )(fill_count, dispatched.reshape(S, E, C // SUB, SUB, D), w_gate, w_up, w_down)


def index_kernel(bounds, counts, expert_ref, slot_ref, idx_ref, total_ref, which_ref, held, rank):
    group, E = counts.shape[0], held.shape[0]
    me = lax.axis_index("ep")
    ids, place = expert_ref[...], slot_ref[...]
    H = len(HEADS)

    def blocks(d, s, e):
        return (counts[d, s, e] + SUB - 1) // SUB

    def device(d, carry):
        number, most = carry
        for e in range(E):
            held[e] = functools.reduce(lambda u, v: u + v, [blocks(d, s, e) for s in range(group)])
        for e in range(E):
            r = 0
            for k in range(E):
                if k != e:
                    ahead = held[k] >= held[e] if k < e else held[k] > held[e]
                    r = r + ahead.astype(jnp.int32)
            rank[e] = r
        for p in range(H + 1):
            total_ref[p, d] = 0
        for e in range(E):
            n = blocks(d, me, e) * SUB
            before = 0
            for k in range(E):
                if k != e:
                    use = (rank[k] >= H) & (rank[k] < rank[e])
                    before = before + jnp.where(use, blocks(d, me, k) * SUB, 0)
            phase = jnp.minimum(rank[e], H)
            total_ref[phase, d] = total_ref[phase, d] + n
            at = phase * (STRIDE * group) + d * STRIDE + before
            number = jnp.where(ids == d * E + e, at + place, number)
        for s in range(group):
            n = 0
            for e in range(E):
                n = n + jnp.where(rank[e] >= H, blocks(d, s, e), 0)
            most = jnp.maximum(most, n * SUB)
        return number, most

    number, most = lax.fori_loop(0, group, device, (jnp.full(ids.shape, -1, jnp.int32), jnp.int32(0)))
    idx_ref[...] = jnp.where(place >= 0, number, -1)
    which = 0
    for b in bounds[:-1]:
        which = which + (most > b).astype(jnp.int32)
    which_ref[0] = which


def make_index(bounds, E, counts, expert_id, slot_index):
    group = counts.shape[0]
    vmem, smem = pl.BlockSpec(memory_space=pltpu.VMEM), pl.BlockSpec(memory_space=pltpu.SMEM)
    return pl.pallas_call(
        functools.partial(index_kernel, bounds),
        out_shape=(jax.ShapeDtypeStruct(expert_id.shape, jnp.int32),
                   jax.ShapeDtypeStruct((len(HEADS) + 1, group), jnp.int32),
                   jax.ShapeDtypeStruct((1,), jnp.int32)),
        in_specs=[smem, vmem, vmem],
        out_specs=(vmem, smem, smem),
        scratch_shapes=[pltpu.SMEM((E,), jnp.int32), pltpu.SMEM((E,), jnp.int32)],
        cost_estimate=pl.CostEstimate(flops=2000000, bytes_accessed=100000, transcendentals=0),
        name="index",
    )(counts, expert_id, slot_index)


def return_kernel(M, group, heads, total, idx, weight_ref, *refs):
    head_hbm, refs = refs[:heads], refs[heads:]
    y_hbm, out_ref, rb, hb, acc, send_sem, recv_sem, own_sem, head_sem = refs
    me = lax.axis_index("ep")
    C = hb.shape[2] * SUB
    T, D = acc.shape
    J = idx.shape[0]
    barrier(group)
    own = pltpu.make_async_copy(y_hbm.at[me, pl.ds(0, M // SUB)], rb.at[0], own_sem)
    copies = []
    for o in range(1, group):
        to = lax.rem(me + o, group)
        copies.append(pltpu.make_async_remote_copy(
            y_hbm.at[to, pl.ds(0, M // SUB)], rb.at[o], send_sem.at[o], recv_sem.at[o],
            device_id={"ep": to}, device_id_type=MESH))
    for copy in copies:
        copy.start()
    own.start()
    head_copies = [pltpu.make_async_copy(head_hbm[p], hb.at[p], head_sem.at[p]) for p in range(heads)]
    for copy in head_copies:
        copy.start()
    acc[...] = jnp.zeros_like(acc)

    def add(load, size, first, skip, limit):
        at = lax.broadcasted_iota(jnp.int32, (size, T), 0)
        row = jnp.where(at >= skip, at + first, -2)
        w = jnp.zeros((size, T), jnp.float32)
        for j in range(J):
            w = jnp.where(row == idx[j:j + 1, :], weight_ref[j:j + 1, :], w)
        hi = w.astype(jnp.bfloat16)
        rest = w - hi.astype(jnp.float32)
        mid = rest.astype(jnp.bfloat16)
        lo = (rest - mid.astype(jnp.float32)).astype(jnp.bfloat16)
        p3 = jnp.concatenate([hi, mid, lo], axis=0)
        alive = lax.broadcasted_iota(jnp.int32, (size, 256), 0) < limit
        for n in range(D // 256):
            cols = pl.ds(n * 256, 256)
            y = jnp.where(alive, load(cols).astype(jnp.float32), 0.0).astype(jnp.bfloat16)
            y3 = jnp.concatenate([y, y, y], axis=0)
            acc[:, cols] += lax.dot_general(p3, y3, (((0,), (0,)), ((), ())), preferred_element_type=jnp.float32)

    for p in range(heads):
        head_copies[p].wait()

    def head(i, c):
        p, d = i // group, lax.rem(i, group)
        add(lambda cols: hb[p, d, :, :, cols].reshape(C, 256), C, (p * group + d) * STRIDE, 0, total[p, d])
        return c

    lax.fori_loop(0, heads * group, head, 0)
    own.wait()
    size = min(KB, M)

    def step(o, c):
        d = lax.rem(me - o + group, group)

        @pl.when(o > 0)
        def _():
            copy = pltpu.make_async_remote_copy(
                y_hbm.at[0, pl.ds(0, M // SUB)], rb.at[o], send_sem.at[o], recv_sem.at[o],
                device_id={"ep": lax.rem(me + jnp.maximum(o, 1), group)}, device_id_type=MESH)
            copy.wait()

        def block(i, c):
            r0 = jnp.minimum(i * size, M - size)
            add(lambda cols: rb[o, pl.ds(r0 // SUB, size // SUB), :, cols].reshape(size, 256), size,
                (heads * group + d) * STRIDE + r0, i * size - r0, total[heads, d] - r0)
            return c

        lax.fori_loop(0, -(-M // size), block, 0)
        return c

    lax.fori_loop(0, group, step, 0)
    out_ref[...] = acc[...].astype(out_ref.dtype)


def return_rows(M, cid, total, idx, gate_weight, *ys):
    heads = len(ys) - 1
    group = total.shape[1]
    _, T = idx.shape
    D = ys[0].shape[-1]
    vmem, hbm = pl.BlockSpec(memory_space=pltpu.VMEM), pl.BlockSpec(memory_space=pltpu.HBM)
    return pl.pallas_call(
        functools.partial(return_kernel, M, group, heads),
        out_shape=jax.ShapeDtypeStruct((T, D), jnp.bfloat16),
        in_specs=[pl.BlockSpec(memory_space=pltpu.SMEM), vmem, vmem] + [hbm] * len(ys),
        out_specs=vmem,
        scratch_shapes=[
            pltpu.VMEM((group, M // SUB, SUB, D), jnp.bfloat16),
            pltpu.VMEM((heads,) + ys[0].shape, jnp.bfloat16),
            pltpu.VMEM((T, D), jnp.float32),
            pltpu.SemaphoreType.DMA((group,)),
            pltpu.SemaphoreType.DMA((group,)),
            pltpu.SemaphoreType.DMA,
            pltpu.SemaphoreType.DMA((heads,)),
        ],
        compiler_params=pltpu.CompilerParams(collective_id=cid, has_side_effects=True, vmem_limit_bytes=VMEM_LIMIT),
    )(total, idx, gate_weight, *ys)


HEADS = (0, 1)
BOUNDS = (72, 88, 104, 120, 136, 152, 168, 184, 216, 288, 384)


def solution(mesh):
    group = mesh.shape["ep"]

    def local_step(dispatched, w_gate, w_up, w_down, fill_count, slot_index, expert_id, gate_weight):
        E, C = dispatched.shape[1:3]
        H = len(HEADS)
        top = (E - H) * C
        bounds = tuple(b for b in BOUNDS if b < top) + (top,)
        args = (dispatched, w_gate, w_up, w_down, fill_count)
        heads = []
        for h in HEADS:
            y = ffn(h, h + 1, *args)
            heads.append(lax.all_to_all(y, "ep", 0, 0, tiled=True))
        y = ffn(H, E, *args)
        counts = exchange_counts(fill_count, group)
        idx, total, which = make_index(bounds, E, counts, expert_id.T, slot_index.T)
        branches = [functools.partial(return_rows, b, 1 + i) for i, b in enumerate(bounds)]
        return lax.switch(which[0], branches, total, idx, gate_weight.T, *heads, y)

    token_spec = P(("dp", "ep"))
    in_specs = (P("dp", "ep"), P("ep"), P("ep"), P("ep"), P("dp", "ep"), token_spec, token_spec, token_spec)
    return jax.shard_map(local_step, mesh=mesh, in_specs=in_specs, out_specs=token_spec, check_vma=False)
```

```python
import functools

import jax
import jax.numpy as jnp
from jax import lax
from jax.experimental import pallas as pl
from jax.experimental.pallas import tpu as pltpu
from jax.sharding import PartitionSpec as P

MESH = pl.DeviceIdType.MESH
SUB = 8
TILE, SMALL = 384, 128
WIDE = 256
STRIP = 64
KB = 256
COLS = 256
STRIDE = 1024
VMEM_LIMIT = 66 * 1000 * 1000


def whole(rows):
    return (rows + KB - 1) // KB * KB


def barrier(group):
    me = lax.axis_index("ep")
    sem = pltpu.get_barrier_semaphore()
    for o in range(1, group):
        pl.semaphore_signal(sem, inc=1, device_id={"ep": lax.rem(me + o, group)}, device_id_type=MESH)
    pl.semaphore_wait(sem, group - 1)


def plan_kernel(group, E, bounds, fill_ref, expert_ref, slot_ref, idx_ref, total_ref, which_ref,
                every, send_sem, recv_sem, own_sem):
    me = lax.axis_index("ep")
    barrier(group)
    own = pltpu.make_async_copy(fill_ref, every.at[me], own_sem)
    own.start()
    copies = []
    for o in range(1, group):
        to = lax.rem(me + o, group)
        copy = pltpu.make_async_remote_copy(
            fill_ref, every.at[me], send_sem.at[o], recv_sem.at[o], device_id={"ep": to}, device_id_type=MESH)
        copy.start()
        copies.append(copy)
    ids, place = expert_ref[...], slot_ref[...]
    number = jnp.full(ids.shape, -1, jnp.int32)
    H = len(HEADS)
    lane = lax.broadcasted_iota(jnp.int32, (group, 128), 1)
    row = lax.broadcasted_iota(jnp.int32, (group, 128), 0)
    own.wait()
    for copy in copies:
        copy.wait()
    rows = [(every[d] + (SUB - 1)) // SUB * SUB for d in range(group)]
    held = functools.reduce(lambda u, v: u + v, [
        jnp.where(row == d, jnp.sum(rows[d], axis=0, keepdims=True), 0) for d in range(group)])
    mine = functools.reduce(lambda u, v: u + v, [
        jnp.where(row == d, jnp.sum(jnp.where(row == me, rows[d], 0), axis=0, keepdims=True), 0) for d in range(group)])
    rank = jnp.zeros_like(held)
    for k in range(E):
        other = held[:, k:k + 1]
        rank = rank + jnp.where((other > held) | ((other == held) & (k < lane)), 1, 0)
    before = jnp.zeros_like(held)
    for k in range(E):
        rk = rank[:, k:k + 1]
        before = before + jnp.where((rk >= H) & (rk < rank), mine[:, k:k + 1], 0)
    first = jnp.minimum(rank, H) * (STRIDE * group) + row * STRIDE + before
    most = jnp.zeros((group, 1), jnp.int32)
    for d in range(group):
        rest = jnp.where((rank[d:d + 1, :] >= H) & (lane < E), rows[d], 0)
        most = jnp.maximum(most, jnp.sum(rest, axis=1, keepdims=True))
    most = jnp.max(jnp.broadcast_to(most, (group, 128)), axis=0, keepdims=True)
    which = jnp.zeros_like(most)
    for b in bounds[:-1]:
        which = which + jnp.where(most > b, 1, 0)
    which_ref[...] = jnp.broadcast_to(which, which_ref.shape)
    total = jnp.zeros_like(held)
    for p in range(H + 1):
        here = jnp.where((jnp.minimum(rank, H) == p) & (lane < E), mine, 0)
        total = jnp.where(lane == p, jnp.sum(here, axis=1, keepdims=True), total)
    total_ref[...] = total
    for d in range(group):
        for e in range(E):
            number = jnp.where(ids == d * E + e, first[d:d + 1, e:e + 1], number)
    idx_ref[...] = jnp.where(place >= 0, number + place, -1)


def make_plan(bounds, group, fill_count, expert_id, slot_index):
    E = fill_count.shape[1]
    block = jnp.pad(fill_count, ((0, 0), (0, 128 - E)))
    vmem = pl.BlockSpec(memory_space=pltpu.VMEM)
    return pl.pallas_call(
        functools.partial(plan_kernel, group, E, bounds),
        out_shape=(jax.ShapeDtypeStruct(expert_id.shape, jnp.int32),
                   jax.ShapeDtypeStruct((group, 128), jnp.int32),
                   jax.ShapeDtypeStruct((group, 128), jnp.int32)),
        in_specs=[vmem] * 3,
        out_specs=(vmem,) * 3,
        scratch_shapes=[pltpu.VMEM((group,) + block.shape, jnp.int32),
                        pltpu.SemaphoreType.DMA((group,)), pltpu.SemaphoreType.DMA((group,)), pltpu.SemaphoreType.DMA],
        compiler_params=pltpu.CompilerParams(collective_id=0, has_side_effects=True),
        name="plan",
    )(block, expert_id, slot_index)


def ffn_kernel(S, E, i0, i1, fill_ref, x_hbm, wg_hbm, wu_hbm, wd_hbm, y_hbm,
               xb, wg, wu, wd, hb, yb, live, pos, order, x_sem, w_sem, y_sem):
    F = wg.shape[2]
    D = wg.shape[1]
    alone = i1 == i0 + 1
    steps = F // WIDE
    tail = F - steps * WIDE
    cuts = (0, WIDE, (steps // 2 + 1) * WIDE, F)
    parts = tuple((p, q - p) for p, q in zip(cuts, cuts[1:]))

    def blocks(s, e):
        return (fill_ref[s, e] + SUB - 1) // SUB

    held = [functools.reduce(lambda u, v: u + v, [blocks(s, e) for s in range(S)]) for e in range(E)]
    for e in range(E):
        rank = 0
        for k in range(E):
            if k != e:
                ahead = held[k] >= held[e] if k < e else held[k] > held[e]
                rank = rank + ahead.astype(jnp.int32)
        order[rank] = e

    def weight_copies(e, slot):
        out = []
        for p, (a, n) in enumerate(parts):
            cols = pl.ds(a, n)
            out.append(pltpu.make_async_copy(wg_hbm.at[e, :, cols], wg.at[slot, :, cols], w_sem.at[slot, 2 * p]))
            out.append(pltpu.make_async_copy(wu_hbm.at[e, :, cols], wu.at[slot, :, cols], w_sem.at[slot, 2 * p + 1]))
        out.append(pltpu.make_async_copy(wd_hbm.at[e], wd.at[slot], w_sem.at[slot, 2 * len(parts)]))
        return out

    def row_copies(e, slot):
        out, at = [], 0
        for s in range(S):
            n = blocks(s, e)
            out.append(pltpu.make_async_copy(
                x_hbm.at[s, e, pl.ds(0, n)], xb.at[slot, pl.ds(at, n)], x_sem.at[slot, s]))
            at = at + n
        return out, at

    def result_copies(e, slot, read_pos):
        out, at = [], 0
        for s in range(S):
            n = blocks(s, e)
            out.append(pltpu.make_async_copy(
                yb.at[slot, pl.ds(at, n)], y_hbm.at[s, pl.ds(read_pos(s), n)], y_sem.at[slot, s]))
            at = at + n
        return out

    def fetch(e, slot):
        copies, _ = row_copies(e, slot)
        for c in copies:
            c.start()
        for c in weight_copies(e, slot):
            c.start()

    def fetch_first(e):
        copies, _ = row_copies(e, 0)
        for c in copies:
            c.start()
        for c in weight_copies(e, 0)[:4 if alone else None]:
            c.start()

    fetch_first(order[i0])
    for s in range(S):
        pos[0, s] = 0

    def expert(i, carry):
        e = order[i]
        slot = lax.rem(i - i0, 2)

        copies, total = row_copies(e, slot)
        for c in copies:
            c.wait()
        weights = weight_copies(e, slot)

        @pl.when(i + 1 < i1)
        def _():
            fetch(order[i + 1], 1 - slot)

        @pl.when(i >= i0 + 2)
        def _():
            for c in result_copies(order[i - 2], slot, lambda s: pos[1 + slot, s]):
                c.wait()

        rows = total * SUB

        def up(b0, tile, c, k):
            cols = pl.ds(c, k)
            x = xb[slot, pl.ds(b0, tile // SUB)].reshape(tile, D)
            w = jnp.concatenate([wg[slot, :, cols], wu[slot, :, cols]], axis=1)
            ab = jnp.dot(x, w, preferred_element_type=jnp.float32)
            on = live[pl.ds(0, tile), :] > 0
            for q in range(0, k, 128):
                a, b = ab[:, q:q + 128], ab[:, k + q:k + q + 128]
                h = jnp.where(on, a * jax.nn.sigmoid(a) * b, 0.0)
                hb[pl.ds(0, tile), pl.ds(c + q, 128)] = h.astype(jnp.bfloat16)

        def down(b0, tile, c):
            cols = pl.ds(c * 512 if isinstance(c, int) else pl.multiple_of(c * 512, 512), 512)
            y = jnp.dot(hb[pl.ds(0, tile), :], wd[slot, :, cols], preferred_element_type=jnp.float32)
            yb[slot, pl.ds(b0, tile // SUB), :, cols] = y.astype(jnp.bfloat16).reshape(tile // SUB, SUB, 512)

        def mask(b0, tile):
            row = lax.broadcasted_iota(jnp.int32, (tile, 128), 0) + b0 * SUB
            ok = jnp.zeros((tile, 128), jnp.int32)
            at = 0
            for s in range(S):
                ok = jnp.where((row >= at * SUB) & (row < at * SUB + fill_ref[s, e]), 1, ok)
                at = at + blocks(s, e)
            live[pl.ds(0, tile), :] = ok

        def run(b0, tile, first):
            mask(b0, tile)

            def step(c, carry):
                for p, (at, _) in enumerate(parts):
                    if isinstance(c, int) and c * WIDE != at:
                        continue

                    @pl.when(first & (c * WIDE == at))
                    def _():
                        weights[2 * p].wait()
                        weights[2 * p + 1].wait()

                        if alone:
                            for w in weights[2 * p + 4:2 * p + 6]:
                                w.start()
                up(b0, tile, c * WIDE if isinstance(c, int) else pl.multiple_of(c * WIDE, WIDE), WIDE)
                return carry

            if tile == SMALL and not alone:
                for c in range(steps):
                    step(c, 0)
            else:
                lax.fori_loop(0, steps, step, 0)
            if tail:
                up(b0, tile, steps * WIDE, tail)

            @pl.when(first)
            def _():
                weights[2 * len(parts)].wait()

            def last(c, carry):
                down(b0, tile, c)
                return carry

            if tile == SMALL and not alone:
                for c in range(D // 512):
                    last(c, 0)
            else:
                lax.fori_loop(0, D // 512, last, 0)

        big = (rows + TILE - 1 - 2 * SMALL) // TILE
        rest = jnp.maximum(rows - big * TILE, 0)

        def large(k, c):
            run(k * (TILE // SUB), TILE, k == 0)
            return c

        def small(k, c):
            run(big * (TILE // SUB) + k * (SMALL // SUB), SMALL, (k == 0) & (big == 0))
            return c

        lax.fori_loop(0, big, large, 0)
        lax.fori_loop(0, (rest + SMALL - 1) // SMALL, small, 0)

        for s in range(S):
            pos[1 + slot, s] = pos[0, s]
        for c in result_copies(e, slot, lambda s: pos[1 + slot, s]):
            c.start()
        for s in range(S):
            pos[0, s] = pos[0, s] + blocks(s, e)
        return carry

    lax.fori_loop(i0, i1, expert, 0)
    for i in range(max(i0, i1 - 2), i1):
        for c in result_copies(order[i], (i - i0) % 2, lambda s: pos[1 + (i - i0) % 2, s]):
            c.wait()


def ffn(i0, i1, dispatched, w_gate, w_up, w_down, fill_count):
    S, E, C, D = dispatched.shape
    F = w_gate.shape[2]
    nb = S * C // SUB + TILE // SUB
    parts = 3
    slots = min(2, i1 - i0)
    anyspec = pl.BlockSpec(memory_space=pltpu.HBM)
    return pl.pallas_call(
        functools.partial(ffn_kernel, S, E, i0, i1),
        out_shape=jax.ShapeDtypeStruct((S, (C if i1 == i0 + 1 else whole((i1 - i0) * C)) // SUB, SUB, D), jnp.bfloat16),
        in_specs=[pl.BlockSpec(memory_space=pltpu.SMEM)] + [anyspec] * 4,
        out_specs=anyspec,
        scratch_shapes=[
            pltpu.VMEM((slots, nb, SUB, D), jnp.bfloat16),
            pltpu.VMEM((slots, D, F), jnp.bfloat16),
            pltpu.VMEM((slots, D, F), jnp.bfloat16),
            pltpu.VMEM((slots, F, D), jnp.bfloat16),
            pltpu.VMEM((TILE, F), jnp.bfloat16),
            pltpu.VMEM((slots, nb, SUB, D), jnp.bfloat16),
            pltpu.VMEM((TILE, 128), jnp.int32),
            pltpu.SMEM((3, S), jnp.int32),
            pltpu.SMEM((E,), jnp.int32),
            pltpu.SemaphoreType.DMA((2, S)),
            pltpu.SemaphoreType.DMA((2, 2 * parts + 1)),
            pltpu.SemaphoreType.DMA((2, S)),
        ],
        compiler_params=pltpu.CompilerParams(vmem_limit_bytes=VMEM_LIMIT),
        cost_estimate=pl.CostEstimate(
            flops=6 * S * C * (i1 - i0) * D * F // 2, bytes_accessed=6 * (i1 - i0) * D * F, transcendentals=0),
        name="ffn_%d" % i0,
    )(fill_count, dispatched.reshape(S, E, C // SUB, SUB, D), w_gate, w_up, w_down)


def return_kernel(M, group, heads, total, idx, weight_ref, *refs):
    head_hbm, refs = refs[:heads], refs[heads:]
    y_hbm, out_ref, rb, hb, acc, column, wide_idx, wide_w, p3, send_sem, recv_sem, own_sem, head_sem = refs
    me = lax.axis_index("ep")
    C = hb.shape[2] * SUB
    T, D = acc.shape
    J = idx.shape[0]
    barrier(group)
    own = pltpu.make_async_copy(y_hbm.at[me, pl.ds(0, M // SUB)], rb.at[0], own_sem)
    copies = []
    for o in range(1, group):
        to = lax.rem(me + o, group)
        copies.append(pltpu.make_async_remote_copy(
            y_hbm.at[to, pl.ds(0, M // SUB)], rb.at[o], send_sem.at[o], recv_sem.at[o],
            device_id={"ep": to}, device_id_type=MESH))
    for copy in copies:
        copy.start()
    own.start()
    head_copies = [pltpu.make_async_copy(head_hbm[p], hb.at[p], head_sem.at[p]) for p in range(heads)]
    for copy in head_copies:
        copy.start()

    flat = jnp.concatenate([idx[...].astype(jnp.float32), weight_ref[...], jnp.zeros((16 - 2 * J, T), jnp.float32)], axis=0)
    flat = jnp.transpose(jnp.concatenate([flat, jnp.zeros((112, T), jnp.float32)], axis=0))
    column[...] = flat

    def strip(i, c):
        part = pl.ds(pl.multiple_of(i * STRIP, STRIP), STRIP)
        for j in range(J):
            wide_idx[j, part, :] = jnp.broadcast_to(column[part, j:j + 1], (STRIP, 128)).astype(jnp.int32)
            wide_w[j, part, :] = jnp.broadcast_to(column[part, J + j:J + j + 1], (STRIP, 128))
        acc[part, :] = jnp.zeros((STRIP, D), jnp.float32)
        return c

    lax.fori_loop(0, T // STRIP, strip, 0)

    def add(load, first, limits, size):
        count = len(limits) * size
        width = -(-count // 128) * 128
        strips = T // STRIP

        def pick(i, carry):
            c = pl.multiple_of(i // strips * 128, 128)
            part = pl.ds(pl.multiple_of(lax.rem(i, strips) * STRIP, STRIP), STRIP)
            lane = lax.broadcasted_iota(jnp.int32, (1, 128), 1) + c
            row = lane + first[0]
            for g in range(1, len(limits)):
                row = jnp.where(lane >= g * size, lane + (first[g] - g * size), row)
            row = jnp.where(lane < count, row, -2)
            w = jnp.zeros((STRIP, 128), jnp.float32)
            for j in range(J):
                w = jnp.where(row == wide_idx[j, part, :], wide_w[j, part, :], w)
            hi = w.astype(jnp.bfloat16)
            rest = w - hi.astype(jnp.float32)
            mid = rest.astype(jnp.bfloat16)
            lo = (rest - mid.astype(jnp.float32)).astype(jnp.bfloat16)
            for q, v in enumerate((hi, mid, lo)):
                p3[part, pl.ds(pl.multiple_of(q * width + c, 128), 128)] = v
            return carry

        lax.fori_loop(0, width // 128 * strips, pick, 0)

        def columns(n, c):
            cols = pl.ds(pl.multiple_of(n * COLS, COLS), COLS)
            ys = []
            for g, limit in enumerate(limits):
                alive = lax.broadcasted_iota(jnp.int32, (size, COLS), 0) < limit
                ys.append(jnp.where(alive, load(g, cols).astype(jnp.float32), 0.0).astype(jnp.bfloat16))
            if width > count:
                ys.append(jnp.zeros((width - count, COLS), jnp.bfloat16))
            y3 = jnp.concatenate(ys * 3, axis=0)
            acc[:, cols] += jnp.dot(p3[:, :3 * width], y3, preferred_element_type=jnp.float32)
            return c

        lax.fori_loop(0, D // COLS, columns, 0)

    for p in range(heads):
        head_copies[p].wait()
    four = 4 if group % 4 == 0 else 1

    def head(i, c):
        p, d0 = four * i // group, lax.rem(four * i, group)
        add(lambda g, cols: hb[p, d0 + g, :, :, cols].reshape(C, COLS),
            [(p * group + d0 + g) * STRIDE for g in range(four)], [total[d0 + g, p] for g in range(four)], C)
        return c

    lax.fori_loop(0, heads * group // four, head, 0)
    own.wait()
    size = min(M, KB)
    pair = 2 if 2 * size <= 256 and group % 2 == 0 else 1

    def step(i, c):
        for g in range(pair):
            o = i * pair + g

            @pl.when(o > 0)
            def _():
                copy = pltpu.make_async_remote_copy(
                    y_hbm.at[0, pl.ds(0, M // SUB)], rb.at[o], send_sem.at[o], recv_sem.at[o],
                    device_id={"ep": lax.rem(me + jnp.maximum(o, 1), group)}, device_id_type=MESH)
                copy.wait()
        ds = [lax.rem(me - i * pair - g + group, group) for g in range(pair)]

        def block(k, c):
            r0 = k * size
            add(lambda g, cols: rb[i * pair + g, pl.ds(r0 // SUB, size // SUB), :, cols].reshape(size, COLS),
                [(heads * group + d) * STRIDE + r0 for d in ds], [total[d, heads] - r0 for d in ds], size)
            return c
        if M > size:
            lax.fori_loop(0, M // size, block, 0)
        else:
            block(0, 0)
        return c

    lax.fori_loop(0, group // pair, step, 0)

    def finish(i, c):
        part = pl.ds(pl.multiple_of(i * STRIP, STRIP), STRIP)
        out_ref[part, :] = acc[part, :].astype(out_ref.dtype)
        return c

    lax.fori_loop(0, T // STRIP, finish, 0)


def return_rows(M, cid, total, idx, gate_weight, *ys):
    heads = len(ys) - 1
    group = total.shape[0]
    J, T = idx.shape
    D = ys[0].shape[-1]
    vmem, hbm = pl.BlockSpec(memory_space=pltpu.VMEM), pl.BlockSpec(memory_space=pltpu.HBM)
    return pl.pallas_call(
        functools.partial(return_kernel, M, group, heads),
        out_shape=jax.ShapeDtypeStruct((T, D), jnp.bfloat16),
        in_specs=[pl.BlockSpec(memory_space=pltpu.SMEM), vmem, vmem] + [hbm] * len(ys),
        out_specs=vmem,
        scratch_shapes=[
            pltpu.VMEM((group, M // SUB, SUB, D), jnp.bfloat16),
            pltpu.VMEM((heads,) + ys[0].shape, jnp.bfloat16),
            pltpu.VMEM((T, D), jnp.float32),
            pltpu.VMEM((T, 128), jnp.float32),
            pltpu.VMEM((J, T, 128), jnp.int32),
            pltpu.VMEM((J, T, 128), jnp.float32),
            pltpu.VMEM((T, 3 * 384), jnp.bfloat16),
            pltpu.SemaphoreType.DMA((group,)),
            pltpu.SemaphoreType.DMA((group,)),
            pltpu.SemaphoreType.DMA,
            pltpu.SemaphoreType.DMA((heads,)),
        ],
        compiler_params=pltpu.CompilerParams(collective_id=cid, has_side_effects=True, vmem_limit_bytes=VMEM_LIMIT),
        name="return_%d" % M,
    )(total, idx, gate_weight, *ys)


HEADS = (0, 1)
BOUNDS = (80, 96, 112, 128, 160, 176, 192, 256)


def solution(mesh):
    group = mesh.shape["ep"]

    def local_step(dispatched, w_gate, w_up, w_down, fill_count, slot_index, expert_id, gate_weight):
        E, C = dispatched.shape[1:3]
        H = len(HEADS)
        top = (E - H) * C
        bounds = tuple(b for b in BOUNDS if b < top) + (whole(top),)
        idx, total, which = make_plan(bounds, group, fill_count, expert_id.T, slot_index.T)
        fill_count, idx, total, which = lax.optimization_barrier((fill_count, idx, total, which))
        args = (dispatched, w_gate, w_up, w_down, fill_count)
        heads = [lax.all_to_all(ffn(h, h + 1, *args), "ep", 0, 0, tiled=True) for h in HEADS]
        y = ffn(H, E, *args)
        branches = [functools.partial(return_rows, b, 1 + i) for i, b in enumerate(bounds)]
        return lax.switch(which[0, 0], branches, total, idx, gate_weight.T, *heads, y)

    token_spec = P(("dp", "ep"))
    in_specs = (P("dp", "ep"), P("ep"), P("ep"), P("ep"), P("dp", "ep"), token_spec, token_spec, token_spec)
    return jax.shard_map(local_step, mesh=mesh, in_specs=in_specs, out_specs=token_spec, check_vma=False)
```

```python
import functools

import jax
import jax.numpy as jnp
from jax import lax
from jax.experimental import pallas as pl
from jax.experimental.pallas import tpu as pltpu
from jax.sharding import PartitionSpec as P

MESH = pl.DeviceIdType.MESH
SUB = 8
TILE, SMALL = 384, 128
WIDE = 256
STRIP = 128
KB = 256
COLS = 512
STRIDE = 1024
VMEM_LIMIT = 66 * 1000 * 1000


def whole(rows):
    return (rows + KB - 1) // KB * KB


def barrier(group):
    me = lax.axis_index("ep")
    sem = pltpu.get_barrier_semaphore()
    for o in range(1, group):
        pl.semaphore_signal(sem, inc=1, device_id={"ep": lax.rem(me + o, group)}, device_id_type=MESH)
    pl.semaphore_wait(sem, group - 1)


def plan_kernel(group, E, bounds, fill_ref, expert_ref, slot_ref, idx_ref, total_ref, which_ref,
                every, send_sem, recv_sem, own_sem):
    me = lax.axis_index("ep")
    barrier(group)
    own = pltpu.make_async_copy(fill_ref, every.at[me], own_sem)
    own.start()
    copies = []
    for o in range(1, group):
        to = lax.rem(me + o, group)
        copy = pltpu.make_async_remote_copy(
            fill_ref, every.at[me], send_sem.at[o], recv_sem.at[o], device_id={"ep": to}, device_id_type=MESH)
        copy.start()
        copies.append(copy)
    ids, place = expert_ref[...], slot_ref[...]
    number = jnp.full(ids.shape, -1, jnp.int32)
    H = len(HEADS)
    lane = lax.broadcasted_iota(jnp.int32, (group, 128), 1)
    row = lax.broadcasted_iota(jnp.int32, (group, 128), 0)
    own.wait()
    for copy in copies:
        copy.wait()
    rows = [(every[d] + (SUB - 1)) // SUB * SUB for d in range(group)]
    held = functools.reduce(lambda u, v: u + v, [
        jnp.where(row == d, jnp.sum(rows[d], axis=0, keepdims=True), 0) for d in range(group)])
    mine = functools.reduce(lambda u, v: u + v, [
        jnp.where(row == d, jnp.sum(jnp.where(row == me, rows[d], 0), axis=0, keepdims=True), 0) for d in range(group)])
    rank = jnp.zeros_like(held)
    for k in range(E):
        other = held[:, k:k + 1]
        rank = rank + jnp.where((other > held) | ((other == held) & (k < lane)), 1, 0)
    before = jnp.zeros_like(held)
    for k in range(E):
        rk = rank[:, k:k + 1]
        before = before + jnp.where((rk >= H) & (rk < rank), mine[:, k:k + 1], 0)
    first = jnp.minimum(rank, H) * (STRIDE * group) + row * STRIDE + before
    most = jnp.zeros((group, 1), jnp.int32)
    for d in range(group):
        rest = jnp.where((rank[d:d + 1, :] >= H) & (lane < E), rows[d], 0)
        most = jnp.maximum(most, jnp.sum(rest, axis=1, keepdims=True))
    most = jnp.max(jnp.broadcast_to(most, (group, 128)), axis=0, keepdims=True)
    which = jnp.zeros_like(most)
    for b in bounds[:-1]:
        which = which + jnp.where(most > b, 1, 0)
    which_ref[...] = jnp.broadcast_to(which, which_ref.shape)
    total = jnp.zeros_like(held)
    for p in range(H + 1):
        here = jnp.where((jnp.minimum(rank, H) == p) & (lane < E), mine, 0)
        total = jnp.where(lane == p, jnp.sum(here, axis=1, keepdims=True), total)
    total_ref[...] = total
    for d in range(group):
        for e in range(E):
            number = jnp.where(ids == d * E + e, first[d:d + 1, e:e + 1], number)
    idx_ref[...] = jnp.where(place >= 0, number + place, -1)


def make_plan(bounds, group, fill_count, expert_id, slot_index):
    E = fill_count.shape[1]
    block = jnp.pad(fill_count, ((0, 0), (0, 128 - E)))
    vmem = pl.BlockSpec(memory_space=pltpu.VMEM)
    return pl.pallas_call(
        functools.partial(plan_kernel, group, E, bounds),
        out_shape=(jax.ShapeDtypeStruct(expert_id.shape, jnp.int32),
                   jax.ShapeDtypeStruct((group, 128), jnp.int32),
                   jax.ShapeDtypeStruct((group, 128), jnp.int32)),
        in_specs=[vmem] * 3,
        out_specs=(vmem,) * 3,
        scratch_shapes=[pltpu.VMEM((group,) + block.shape, jnp.int32),
                        pltpu.SemaphoreType.DMA((group,)), pltpu.SemaphoreType.DMA((group,)), pltpu.SemaphoreType.DMA],
        compiler_params=pltpu.CompilerParams(collective_id=0, has_side_effects=True),
        name="plan",
    )(block, expert_id, slot_index)


def ffn_kernel(S, E, i0, i1, fill_ref, x_hbm, wg_hbm, wu_hbm, wd_hbm, y_hbm,
               xb, wg, wu, wd, hb, yb, live, pos, order, x_sem, w_sem, y_sem):
    F = wg.shape[2]
    D = wg.shape[1]
    alone = i1 == i0 + 1
    steps = F // WIDE
    tail = F - steps * WIDE
    cuts = (0, WIDE, (steps // 2 + 1) * WIDE, F)
    parts = tuple((p, q - p) for p, q in zip(cuts, cuts[1:]))

    def blocks(s, e):
        return (fill_ref[s, e] + SUB - 1) // SUB

    held = [functools.reduce(lambda u, v: u + v, [blocks(s, e) for s in range(S)]) for e in range(E)]
    for e in range(E):
        rank = 0
        for k in range(E):
            if k != e:
                ahead = held[k] >= held[e] if k < e else held[k] > held[e]
                rank = rank + ahead.astype(jnp.int32)
        order[rank] = e

    def weight_copies(e, slot):
        out = []
        for p, (a, n) in enumerate(parts):
            cols = pl.ds(a, n)
            out.append(pltpu.make_async_copy(wg_hbm.at[e, :, cols], wg.at[slot, :, cols], w_sem.at[slot, 2 * p]))
            out.append(pltpu.make_async_copy(wu_hbm.at[e, :, cols], wu.at[slot, :, cols], w_sem.at[slot, 2 * p + 1]))
        out.append(pltpu.make_async_copy(wd_hbm.at[e], wd.at[slot], w_sem.at[slot, 2 * len(parts)]))
        return out

    def row_copies(e, slot):
        out, at = [], 0
        for s in range(S):
            n = blocks(s, e)
            out.append(pltpu.make_async_copy(
                x_hbm.at[s, e, pl.ds(0, n)], xb.at[slot, pl.ds(at, n)], x_sem.at[slot, s]))
            at = at + n
        return out, at

    def result_copies(e, slot, read_pos):
        out, at = [], 0
        for s in range(S):
            n = blocks(s, e)
            out.append(pltpu.make_async_copy(
                yb.at[slot, pl.ds(at, n)], y_hbm.at[s, pl.ds(read_pos(s), n)], y_sem.at[slot, s]))
            at = at + n
        return out

    def fetch(e, slot):
        copies, _ = row_copies(e, slot)
        for c in copies:
            c.start()
        for c in weight_copies(e, slot):
            c.start()

    def fetch_first(e):
        copies, _ = row_copies(e, 0)
        for c in copies:
            c.start()
        for c in weight_copies(e, 0)[:4 if alone else None]:
            c.start()

    fetch_first(order[i0])
    for s in range(S):
        pos[0, s] = 0

    def expert(i, carry):
        e = order[i]
        slot = lax.rem(i - i0, 2)

        copies, total = row_copies(e, slot)
        for c in copies:
            c.wait()
        weights = weight_copies(e, slot)

        @pl.when(i + 1 < i1)
        def _():
            fetch(order[i + 1], 1 - slot)

        @pl.when(i >= i0 + 2)
        def _():
            for c in result_copies(order[i - 2], slot, lambda s: pos[1 + slot, s]):
                c.wait()

        rows = total * SUB

        def up(b0, tile, c, k):
            cols = pl.ds(c, k)
            x = xb[slot, pl.ds(b0, tile // SUB)].reshape(tile, D)
            w = jnp.concatenate([wg[slot, :, cols], wu[slot, :, cols]], axis=1)
            ab = jnp.dot(x, w, preferred_element_type=jnp.float32)
            on = live[pl.ds(0, tile), :] > 0
            for q in range(0, k, 128):
                a, b = ab[:, q:q + 128], ab[:, k + q:k + q + 128]
                h = jnp.where(on, a * jax.nn.sigmoid(a) * b, 0.0)
                hb[pl.ds(0, tile), pl.ds(c + q, 128)] = h.astype(jnp.bfloat16)

        def down(b0, tile, c):
            cols = pl.ds(c * 512 if isinstance(c, int) else pl.multiple_of(c * 512, 512), 512)
            y = jnp.dot(hb[pl.ds(0, tile), :], wd[slot, :, cols], preferred_element_type=jnp.float32)
            yb[slot, pl.ds(b0, tile // SUB), :, cols] = y.astype(jnp.bfloat16).reshape(tile // SUB, SUB, 512)

        def mask(b0, tile):
            row = lax.broadcasted_iota(jnp.int32, (tile, 128), 0) + b0 * SUB
            ok = jnp.zeros((tile, 128), jnp.int32)
            at = 0
            for s in range(S):
                ok = jnp.where((row >= at * SUB) & (row < at * SUB + fill_ref[s, e]), 1, ok)
                at = at + blocks(s, e)
            live[pl.ds(0, tile), :] = ok

        def run(b0, tile, first):
            mask(b0, tile)

            def step(c, carry):
                for p, (at, _) in enumerate(parts):
                    if isinstance(c, int) and c * WIDE != at:
                        continue

                    @pl.when(first & (c * WIDE == at))
                    def _():
                        weights[2 * p].wait()
                        weights[2 * p + 1].wait()

                        if alone:
                            for w in weights[2 * p + 4:2 * p + 6]:
                                w.start()
                up(b0, tile, c * WIDE if isinstance(c, int) else pl.multiple_of(c * WIDE, WIDE), WIDE)
                return carry

            if tile == SMALL and not alone:
                for c in range(steps):
                    step(c, 0)
            else:
                lax.fori_loop(0, steps, step, 0)
            if tail:
                up(b0, tile, steps * WIDE, tail)

            @pl.when(first)
            def _():
                weights[2 * len(parts)].wait()

            def last(c, carry):
                down(b0, tile, c)
                return carry

            if tile == SMALL and not alone:
                for c in range(D // 512):
                    last(c, 0)
            else:
                lax.fori_loop(0, D // 512, last, 0)

        big = (rows + TILE - 1 - 2 * SMALL) // TILE
        rest = jnp.maximum(rows - big * TILE, 0)

        def large(k, c):
            run(k * (TILE // SUB), TILE, k == 0)
            return c

        def small(k, c):
            run(big * (TILE // SUB) + k * (SMALL // SUB), SMALL, (k == 0) & (big == 0))
            return c

        lax.fori_loop(0, big, large, 0)
        lax.fori_loop(0, (rest + SMALL - 1) // SMALL, small, 0)

        for s in range(S):
            pos[1 + slot, s] = pos[0, s]
        for c in result_copies(e, slot, lambda s: pos[1 + slot, s]):
            c.start()
        for s in range(S):
            pos[0, s] = pos[0, s] + blocks(s, e)
        return carry

    lax.fori_loop(i0, i1, expert, 0)
    for i in range(max(i0, i1 - 2), i1):
        for c in result_copies(order[i], (i - i0) % 2, lambda s: pos[1 + (i - i0) % 2, s]):
            c.wait()


def ffn(i0, i1, dispatched, w_gate, w_up, w_down, fill_count):
    S, E, C, D = dispatched.shape
    F = w_gate.shape[2]
    nb = S * C // SUB + TILE // SUB
    parts = 3
    slots = min(2, i1 - i0)
    anyspec = pl.BlockSpec(memory_space=pltpu.HBM)
    return pl.pallas_call(
        functools.partial(ffn_kernel, S, E, i0, i1),
        out_shape=jax.ShapeDtypeStruct((S, (C if i1 == i0 + 1 else whole((i1 - i0) * C)) // SUB, SUB, D), jnp.bfloat16),
        in_specs=[pl.BlockSpec(memory_space=pltpu.SMEM)] + [anyspec] * 4,
        out_specs=anyspec,
        scratch_shapes=[
            pltpu.VMEM((slots, nb, SUB, D), jnp.bfloat16),
            pltpu.VMEM((slots, D, F), jnp.bfloat16),
            pltpu.VMEM((slots, D, F), jnp.bfloat16),
            pltpu.VMEM((slots, F, D), jnp.bfloat16),
            pltpu.VMEM((TILE, F), jnp.bfloat16),
            pltpu.VMEM((slots, nb, SUB, D), jnp.bfloat16),
            pltpu.VMEM((TILE, 128), jnp.int32),
            pltpu.SMEM((3, S), jnp.int32),
            pltpu.SMEM((E,), jnp.int32),
            pltpu.SemaphoreType.DMA((2, S)),
            pltpu.SemaphoreType.DMA((2, 2 * parts + 1)),
            pltpu.SemaphoreType.DMA((2, S)),
        ],
        compiler_params=pltpu.CompilerParams(vmem_limit_bytes=VMEM_LIMIT),
        cost_estimate=pl.CostEstimate(
            flops=6 * S * C * (i1 - i0) * D * F // 2, bytes_accessed=6 * (i1 - i0) * D * F, transcendentals=0),
        name="ffn_%d" % i0,
    )(fill_count, dispatched.reshape(S, E, C // SUB, SUB, D), w_gate, w_up, w_down)


def return_kernel(M, group, heads, total, idx, weight_ref, *refs):
    head_hbm, refs = refs[:heads], refs[heads:]
    y_hbm, out_ref, rb, hb, acc, column, wide_idx, wide_w, p3, send_sem, recv_sem, own_sem, head_sem = refs
    me = lax.axis_index("ep")
    C = hb.shape[2] * SUB
    T, D = acc.shape
    J = idx.shape[0]
    barrier(group)
    own = pltpu.make_async_copy(y_hbm.at[me, pl.ds(0, M // SUB)], rb.at[0], own_sem)
    copies = []
    for o in range(1, group):
        to = lax.rem(me + o, group)
        copies.append(pltpu.make_async_remote_copy(
            y_hbm.at[to, pl.ds(0, M // SUB)], rb.at[o], send_sem.at[o], recv_sem.at[o],
            device_id={"ep": to}, device_id_type=MESH))
    for copy in copies:
        copy.start()
    own.start()
    head_copies = [pltpu.make_async_copy(head_hbm[p], hb.at[p], head_sem.at[p]) for p in range(heads)]
    for copy in head_copies:
        copy.start()

    flat = jnp.concatenate([idx[...].astype(jnp.float32), weight_ref[...], jnp.zeros((16 - 2 * J, T), jnp.float32)], axis=0)
    flat = jnp.transpose(jnp.concatenate([flat, jnp.zeros((112, T), jnp.float32)], axis=0))
    column[...] = flat

    def strip(i, c):
        part = pl.ds(pl.multiple_of(i * STRIP, STRIP), STRIP)
        for j in range(J):
            wide_idx[j, part, :] = jnp.broadcast_to(column[part, j:j + 1], (STRIP, 128)).astype(jnp.int32)
            wide_w[j, part, :] = jnp.broadcast_to(column[part, J + j:J + j + 1], (STRIP, 128))
        acc[part, :] = jnp.zeros((STRIP, D), jnp.float32)
        return c

    lax.fori_loop(0, T // STRIP, strip, 0)

    def add(load, first, limits, size):
        count = len(limits) * size
        width = -(-count // 128) * 128
        strips = T // STRIP

        def pick(i, carry):
            c = pl.multiple_of(i // strips * 128, 128)
            part = pl.ds(pl.multiple_of(lax.rem(i, strips) * STRIP, STRIP), STRIP)
            lane = lax.broadcasted_iota(jnp.int32, (1, 128), 1) + c
            row = lane + first[0]
            for g in range(1, len(limits)):
                row = jnp.where(lane >= g * size, lane + (first[g] - g * size), row)
            row = jnp.where(lane < count, row, -2)
            w = jnp.zeros((STRIP, 128), jnp.float32)
            for j in range(J):
                w = jnp.where(row == wide_idx[j, part, :], wide_w[j, part, :], w)
            hi = w.astype(jnp.bfloat16)
            rest = w - hi.astype(jnp.float32)
            mid = rest.astype(jnp.bfloat16)
            lo = (rest - mid.astype(jnp.float32)).astype(jnp.bfloat16)
            for q, v in enumerate((hi, mid, lo)):
                p3[part, pl.ds(pl.multiple_of(q * width + c, 128), 128)] = v
            return carry

        lax.fori_loop(0, width // 128 * strips, pick, 0)

        def columns(n, c):
            cols = pl.ds(pl.multiple_of(n * COLS, COLS), COLS)
            ys = []
            for g, limit in enumerate(limits):
                alive = lax.broadcasted_iota(jnp.int32, (size, COLS), 0) < limit
                ys.append(jnp.where(alive, load(g, cols).astype(jnp.float32), 0.0).astype(jnp.bfloat16))
            if width > count:
                ys.append(jnp.zeros((width - count, COLS), jnp.bfloat16))
            y3 = jnp.concatenate(ys * 3, axis=0)
            acc[:, cols] += jnp.dot(p3[:, :3 * width], y3, preferred_element_type=jnp.float32)
            return c

        lax.fori_loop(0, D // COLS, columns, 0)

    for p in range(heads):
        head_copies[p].wait()
    four = 4 if group % 4 == 0 else 1

    def head(i, c):
        p, d0 = four * i // group, lax.rem(four * i, group)
        add(lambda g, cols: hb[p, d0 + g, :, :, cols].reshape(C, COLS),
            [(p * group + d0 + g) * STRIDE for g in range(four)], [total[d0 + g, p] for g in range(four)], C)
        return c

    lax.fori_loop(0, heads * group // four, head, 0)
    own.wait()
    size = min(M, KB)
    pair = 2 if 2 * size <= 256 and group % 2 == 0 else 1

    def step(i, c):
        for g in range(pair):
            o = i * pair + g

            @pl.when(o > 0)
            def _():
                copy = pltpu.make_async_remote_copy(
                    y_hbm.at[0, pl.ds(0, M // SUB)], rb.at[o], send_sem.at[o], recv_sem.at[o],
                    device_id={"ep": lax.rem(me + jnp.maximum(o, 1), group)}, device_id_type=MESH)
                copy.wait()
        ds = [lax.rem(me - i * pair - g + group, group) for g in range(pair)]

        def block(k, c):
            r0 = k * size
            add(lambda g, cols: rb[i * pair + g, pl.ds(r0 // SUB, size // SUB), :, cols].reshape(size, COLS),
                [(heads * group + d) * STRIDE + r0 for d in ds], [total[d, heads] - r0 for d in ds], size)
            return c
        if M > size:
            lax.fori_loop(0, M // size, block, 0)
        else:
            block(0, 0)
        return c

    lax.fori_loop(0, group // pair, step, 0)

    def finish(i, c):
        part = pl.ds(pl.multiple_of(i * STRIP, STRIP), STRIP)
        out_ref[part, :] = acc[part, :].astype(out_ref.dtype)
        return c

    lax.fori_loop(0, T // STRIP, finish, 0)


def return_rows(M, cid, total, idx, gate_weight, *ys):
    heads = len(ys) - 1
    group = total.shape[0]
    J, T = idx.shape
    D = ys[0].shape[-1]
    vmem, hbm = pl.BlockSpec(memory_space=pltpu.VMEM), pl.BlockSpec(memory_space=pltpu.HBM)
    return pl.pallas_call(
        functools.partial(return_kernel, M, group, heads),
        out_shape=jax.ShapeDtypeStruct((T, D), jnp.bfloat16),
        in_specs=[pl.BlockSpec(memory_space=pltpu.SMEM), vmem, vmem] + [hbm] * len(ys),
        out_specs=vmem,
        scratch_shapes=[
            pltpu.VMEM((group, M // SUB, SUB, D), jnp.bfloat16),
            pltpu.VMEM((heads,) + ys[0].shape, jnp.bfloat16),
            pltpu.VMEM((T, D), jnp.float32),
            pltpu.VMEM((T, 128), jnp.float32),
            pltpu.VMEM((J, T, 128), jnp.int32),
            pltpu.VMEM((J, T, 128), jnp.float32),
            pltpu.VMEM((T, 3 * 384), jnp.bfloat16),
            pltpu.SemaphoreType.DMA((group,)),
            pltpu.SemaphoreType.DMA((group,)),
            pltpu.SemaphoreType.DMA,
            pltpu.SemaphoreType.DMA((heads,)),
        ],
        compiler_params=pltpu.CompilerParams(collective_id=cid, has_side_effects=True, vmem_limit_bytes=VMEM_LIMIT),
        name="return_%d" % M,
    )(total, idx, gate_weight, *ys)


HEADS = (0, 1, 2)
BOUNDS = (64, 80, 96, 112, 128, 160, 192, 256)


def solution(mesh):
    group = mesh.shape["ep"]

    def local_step(dispatched, w_gate, w_up, w_down, fill_count, slot_index, expert_id, gate_weight):
        E, C = dispatched.shape[1:3]
        H = len(HEADS)
        top = (E - H) * C
        bounds = tuple(b for b in BOUNDS if b < top) + (whole(top),)
        idx, total, which = make_plan(bounds, group, fill_count, expert_id.T, slot_index.T)
        fill_count, idx, total, which = lax.optimization_barrier((fill_count, idx, total, which))
        args = (dispatched, w_gate, w_up, w_down, fill_count)
        heads = [lax.all_to_all(ffn(h, h + 1, *args), "ep", 0, 0, tiled=True) for h in HEADS]
        y = ffn(H, E, *args)
        branches = [functools.partial(return_rows, b, 1 + i) for i, b in enumerate(bounds)]
        return lax.switch(which[0, 0], branches, total, idx, gate_weight.T, *heads, y)

    token_spec = P(("dp", "ep"))
    in_specs = (P("dp", "ep"), P("ep"), P("ep"), P("ep"), P("dp", "ep"), token_spec, token_spec, token_spec)
    return jax.shard_map(local_step, mesh=mesh, in_specs=in_specs, out_specs=token_spec, check_vma=False)
```
